32 devices in a mesh: dp: 4 (over y, z), tp: 8 (over x, core).
Axes of the slice: x: 4, y: 2, z: 2, core: 2. Of those that a mesh axis runs over, the one named last changes fastest.
The devices are a block of a 4x4x8 slice.
Arguments:
- x: bfloat16 [12288, 4096], P('dp'), parts along dimension 0
- lens: int32 [8], P('dp'), parts along dimension 0
- g1: bfloat16 [4096], replicated
- g2: bfloat16 [4096], replicated
- wq: bfloat16 [4096, 4096], P(None, 'tp')
- wk: bfloat16 [4096, 1024], replicated
- wv: bfloat16 [4096, 1024], replicated
- wo: bfloat16 [4096, 4096], P('tp')
- wg: bfloat16 [4096, 14336], P(None, 'tp')
- wu: bfloat16 [4096, 14336], P(None, 'tp')
- wd: bfloat16 [14336, 4096], P('tp')
Outputs:
- output 1: bfloat16 [12288, 4096], P('dp'), parts along dimension 0
- output 2: bfloat16 [8, 3072, 8, 128], P('dp', None, 'tp'), parts along dimension 0
- output 3: bfloat16 [8, 3072, 8, 128], P('dp', None, 'tp'), parts along dimension 0
There are 4 independent parts. The reference program is written for one: setup_inputs(seed, part) draws one part's arguments, and reference() takes and returns one part's arrays. A program takes and returns all parts, laid end to end along the dimension named above; an argument that names none is the same for every part.
All inputs are finite; a program needn't handle non-finite values.
Results may differ from the reference program's by a relative error of at most 0.0155253.
Values are sent between devices in bfloat16 or wider.
A program may use at most 768 MiB of HBM per device.

```python
import numpy as np
import jax
import jax.numpy as jnp
from jax import lax

D = 4096
HEADS = 32
KV_HEADS = 8
HEAD = 128
FF = 14336
T = 3072
KVR = 8

QB = min(T, 256)
EPS = 1e-5
BASE = 500000.0


def setup_inputs(seed: int = 0, part: int = 0) -> dict:
    key = jax.random.PRNGKey(seed)
    kp = jax.random.split(jax.random.fold_in(key, part), 4)
    kw = jax.random.split(jax.random.fold_in(key, 1000003), 9)
    kl = jax.random.split(jax.random.fold_in(jax.random.fold_in(key, 7), part), 2)
    t = jnp.arange(T, dtype=jnp.float32)
    freq = jnp.array([1.0, 2.0, 3.0, 5.0], dtype=jnp.float32)
    phase = jax.random.uniform(kp[0], (4,), jnp.float32, 0.0, 2.0 * np.pi)
    amp = 0.5 * jax.random.normal(kp[1], (4, D), jnp.float32)
    wave = jnp.cos(2.0 * np.pi * t[:, None] * freq[None, :] / T + phase[None, :])
    x = jnp.dot(wave, amp) + 0.6 * jax.random.normal(kp[2], (T, D), jnp.float32)
    s = jax.random.randint(kl[0], (), 1, T // 16 + 1, dtype=jnp.int32)
    l1 = jnp.where(jax.random.bernoulli(kl[1]), s, T - s).astype(jnp.int32)
    lens = jnp.stack([l1, T - l1]).astype(jnp.int32)

    def w(k, shape, fan_in, gain=1.0):
        return (gain * fan_in ** -0.5 * jax.random.normal(k, shape, jnp.float32)).astype(jnp.bfloat16)

    return dict(
        x=x.astype(jnp.bfloat16),
        lens=lens,
        g1=(1.0 + 0.2 * jax.random.normal(kw[0], (D,), jnp.float32)).astype(jnp.bfloat16),
        g2=(1.0 + 0.2 * jax.random.normal(kw[1], (D,), jnp.float32)).astype(jnp.bfloat16),
        wq=w(kw[2], (D, HEADS * HEAD), D),
        wk=w(kw[3], (D, KV_HEADS * HEAD), D),
        wv=w(kw[4], (D, KV_HEADS * HEAD), D),
        wo=w(kw[5], (HEADS * HEAD, D), HEADS * HEAD, 2.0),
        wg=w(kw[6], (D, FF), D),
        wu=w(kw[7], (D, FF), D),
        wd=w(kw[8], (FF, D), FF),
    )


def _mm(a, b):
    return jnp.dot(a, b, preferred_element_type=jnp.float32)


def _rms(x, g):
    xf = x.astype(jnp.float32)
    ms = jnp.mean(xf * xf, axis=-1, keepdims=True)
    return (xf * lax.rsqrt(ms + EPS) * g.astype(jnp.float32)).astype(jnp.bfloat16)


def _rope(x, pos):
    inv = BASE ** (-jnp.arange(0, HEAD, 2, dtype=jnp.float32) / HEAD)
    ang = pos.astype(jnp.float32)[:, None] * inv[None, :]
    c = jnp.cos(ang)[:, None, :]
    s = jnp.sin(ang)[:, None, :]
    x1 = x[..., : HEAD // 2]
    x2 = x[..., HEAD // 2 :]
    return jnp.concatenate([x1 * c - x2 * s, x2 * c + x1 * s], axis=-1)


def _attention(q, k, v, seg):
    rep = HEADS // KV_HEADS
    nb = T // QB
    rows = jnp.arange(T)
    qg = jnp.transpose(q.reshape(T, KV_HEADS, rep, HEAD), (1, 0, 2, 3)).astype(jnp.float32)
    kg = jnp.transpose(k, (1, 0, 2)).astype(jnp.float32)
    vg = jnp.transpose(v, (1, 0, 2)).astype(jnp.float32)

    def group(args):
        qh, kh, vh = args

        def block(args2):
            qq, i = args2
            rq = i * QB + jnp.arange(QB)
            s = jnp.einsum('qrd,kd->rqk', qq, kh) * (HEAD ** -0.5)
            mask = (rows[None, :] <= rq[:, None]) & (seg[None, :] == seg[rq][:, None])
            s = jnp.where(mask[None], s, -jnp.inf)
            pr = jax.nn.softmax(s, axis=-1).astype(jnp.bfloat16).astype(jnp.float32)
            return jnp.einsum('rqk,kd->qrd', pr, vh).astype(jnp.bfloat16)

        o = lax.map(block, (qh.reshape(nb, QB, rep, HEAD), jnp.arange(nb)))
        return o.reshape(T, rep, HEAD)

    o = lax.map(group, (qg, kg, vg))
    return jnp.transpose(o, (1, 0, 2, 3)).reshape(T, HEADS * HEAD)


def _cache(k, l1):
    rows = jnp.arange(T)
    z = jnp.zeros((), k.dtype)
    c1 = jnp.where((rows < l1)[:, None, None], k, z)
    c2 = jnp.where((rows < T - l1)[:, None, None], jnp.take(k, (rows + l1) % T, axis=0), z)
    return jnp.stack([c1, c2])


def reference(x, lens, g1, g2, wq, wk, wv, wo, wg, wu, wd):
    l1 = lens[0]
    rows = jnp.arange(T)
    seg = (rows >= l1).astype(jnp.int32)
    pos = jnp.where(seg == 1, rows - l1, rows)
    a = _rms(x, g1)
    q = _rope(_mm(a, wq).reshape(T, HEADS, HEAD), pos).astype(jnp.bfloat16)
    k = _rope(_mm(a, wk).reshape(T, KV_HEADS, HEAD), pos).astype(jnp.bfloat16)
    v = _mm(a, wv).astype(jnp.bfloat16).reshape(T, KV_HEADS, HEAD)
    o = _attention(q, k, v, seg)
    p = _mm(o, wo).astype(jnp.bfloat16)
    h = (x.astype(jnp.float32) + p.astype(jnp.float32)).astype(jnp.bfloat16)
    b = _rms(h, g2)
    gate = _mm(b, wg).astype(jnp.bfloat16)
    up = _mm(b, wu).astype(jnp.bfloat16)
    u = (jax.nn.silu(gate.astype(jnp.float32)) * up.astype(jnp.float32)).astype(jnp.bfloat16)
    r = _mm(u, wd).astype(jnp.bfloat16)
    y = (h.astype(jnp.float32) + r.astype(jnp.float32)).astype(jnp.bfloat16)
    slots = np.arange(KVR) * KV_HEADS // KVR
    return y, _cache(k[:, slots], l1), _cache(v[:, slots], l1)
```

```python
import functools

import jax
import jax.numpy as jnp
from jax import lax
from jax.experimental import pallas as pl
from jax.experimental.pallas import tpu as pltpu
from jax.sharding import PartitionSpec as P

HEAD = 128
EPS = 1e-5
BASE = 500000.0
VMEM_LIMIT = 67000000
F32 = jnp.float32
BF16 = jnp.bfloat16
ANY = pl.BlockSpec(memory_space=pl.ANY)


def _rows_per_chunk(n):
    return 384 if n % 384 == 0 else 128


def _dot(a, b):
    return jnp.dot(a, b, preferred_element_type=F32)


def _cols(i, size):
    return pl.ds(pl.multiple_of(i * size, size), size)


def _rows(i, size):
    return pl.ds(pl.multiple_of(i * size, size), size)


def _norm_chunk(m, x_ref, g, a_ref):
    def body(k, _):
        r = _rows(k, 16)
        xf = x_ref[r, :].astype(F32)
        ms = jnp.mean(xf * xf, axis=-1, keepdims=True)
        a_ref[r, :] = (xf * lax.rsqrt(ms + EPS) * g).astype(BF16)
        return 0

    lax.fori_loop(0, m // 16, body, 0)


def _rope(z, cos, sin):
    return z * cos + pltpu.roll(z, HEAD // 2, 1) * sin


def _project_chunk(i, m, a_ref, wq_ref, wkv_ref, cos_ref, sin_ref, q_ref, k_ref, v_ref):
    a = a_ref[...]
    cos, sin = cos_ref[...], sin_ref[...]
    kv = _dot(a, wkv_ref[...])
    r = _rows(i, m)
    k_ref[r, :] = _rope(kv[:, :HEAD], cos, sin).astype(BF16)
    v_ref[r, :] = kv[:, HEAD:].astype(BF16)
    q = _dot(a, wq_ref[...])
    for h in range(q_ref.shape[0]):
        q_ref[h] = _rope(q[:, h * HEAD:(h + 1) * HEAD], cos, sin).astype(BF16)


def _attend_chunk(i, m, l1, q_ref, k_ref, v_ref, s_ref, o_ref):
    rows = i * m + lax.broadcasted_iota(jnp.int32, (m, 1), 0)
    first = jnp.where(rows >= l1, l1, 0)
    scale = HEAD ** -0.5 * 1.4426950408889634

    def head(h, _):
        q = q_ref[h]

        def score(b, top):
            s = lax.dot_general(q, k_ref[_rows(b, m), :], (((1,), (1,)), ((), ())), preferred_element_type=F32)
            cols = b * m + lax.broadcasted_iota(jnp.int32, (1, m), 1)
            s = jnp.where((cols <= rows) & (cols >= first), s, -jnp.inf)
            s_ref[b] = s
            return jnp.maximum(top, jnp.max(s, axis=1, keepdims=True))

        top = lax.fori_loop(0, i + 1, score, jnp.full((m, 1), -jnp.inf, F32))

        def expo(b, total):
            e = jnp.exp2((s_ref[b] - top) * scale)
            s_ref[b] = e
            return total + jnp.sum(e, axis=1, keepdims=True)

        total = lax.fori_loop(0, i + 1, expo, jnp.zeros((m, 1), F32))
        inv = 1.0 / total

        def value(b, acc):
            return acc + _dot((s_ref[b] * inv).astype(BF16), v_ref[_rows(b, m), :])

        acc = lax.fori_loop(0, i + 1, value, jnp.zeros((m, HEAD), F32))
        o_ref[:, _cols(h, HEAD)] = acc.astype(BF16)
        return 0

    lax.fori_loop(0, q_ref.shape[0], head, 0)


def _attention_kernel(m, l1_ref, x_ref, g_ref, cos_ref, sin_ref, wq_ref, wkv_ref, o_ref, kc_ref, vc_ref,
                      a_buf, q_buf, k_buf, v_buf, s_buf):
    i = pl.program_id(0)
    _norm_chunk(m, x_ref, g_ref[...].astype(F32), a_buf)
    _project_chunk(i, m, a_buf, wq_ref, wkv_ref, cos_ref, sin_ref, q_buf, k_buf, v_buf)
    kc_ref[...] = k_buf[_rows(i, m), :]
    vc_ref[...] = v_buf[_rows(i, m), :]
    _attend_chunk(i, m, l1_ref[0], q_buf, k_buf, v_buf, s_buf, o_ref)


def _attention(x, lens, g1, cos, sin, wq, wkv):
    n, d = x.shape
    m = _rows_per_chunk(n)
    hq = wq.shape[1]
    full = lambda s: pl.BlockSpec(s, lambda i: (0, 0), pipeline_mode=pl.Buffered(buffer_count=1))
    row = lambda c: pl.BlockSpec((m, c), lambda i: (i, 0))
    return pl.pallas_call(
        functools.partial(_attention_kernel, m),
        grid=(n // m,),
        out_shape=(jax.ShapeDtypeStruct((n, hq), BF16), jax.ShapeDtypeStruct((n, HEAD), BF16),
                   jax.ShapeDtypeStruct((n, HEAD), BF16)),
        in_specs=[pl.BlockSpec(memory_space=pltpu.SMEM), row(d), full((1, d)), row(HEAD), row(HEAD),
                  full((d, hq)), full((d, 2 * HEAD))],
        out_specs=(row(hq), row(HEAD), row(HEAD)),
        scratch_shapes=[pltpu.VMEM((m, d), BF16), pltpu.VMEM((hq // HEAD, m, HEAD), BF16),
                        pltpu.VMEM((n, HEAD), BF16), pltpu.VMEM((n, HEAD), BF16),
                        pltpu.VMEM((n // m, m, m), F32)],
        compiler_params=pltpu.CompilerParams(vmem_limit_bytes=VMEM_LIMIT, dimension_semantics=("arbitrary",)),
        name="attention",
    )(lens, x, g1, cos, sin, wq, wkv)


class _Stream:
    def __init__(self, m, part, got, r1l, r1r, r2l, r2r, mine, whole, sems, finish):
        self.m, self.r = m, m // 8
        self.part, self.got, self.mine, self.whole = part, got, mine, whole
        self.r1l, self.r1r, self.r2l, self.r2r = r1l, r1r, r2l, r2r
        self.sems, self.finish = sems, finish
        self.h = part.shape[1] // 2
        t = lax.axis_index("tp")
        x, c = t // 2, t % 2
        self.x, self.c = x, c
        self.xr, self.xo, self.xl = (x + 1) % 4, (x + 2) % 4, (x + 3) % 4
        self.right, self.left = self.xr * 2 + c, self.xl * 2 + c
        self.twin = x * 2 + 1 - c
        self.lo, self.hi = pl.ds(0, self.h), pl.ds(self.h, self.h)

    def send(self, src, dst, k, slot, to):
        return pltpu.make_async_remote_copy(
            src_ref=src, dst_ref=dst, send_sem=self.sems.at[0, slot, k], recv_sem=self.sems.at[1, slot, k],
            device_id={"tp": to}, device_id_type=pl.DeviceIdType.MESH)

    def block(self, chip):
        return pl.ds(pl.multiple_of(chip * self.r, 16), self.r)

    def pair(self, i):
        s = i % 2
        theirs = pl.ds(pl.multiple_of((1 - self.c) * 4 * self.r, 16), 4 * self.r)
        return self.send(self.part.at[theirs, :], self.got.at[s], 0, s, self.twin)

    def first(self, i):
        s = i % 2
        got = self.got.at[s]
        return (
            self.send(got.at[self.block(self.xo), self.lo], self.r1l.at[s, :, self.lo], 1, s, self.right),
            self.send(got.at[self.block(self.xo), self.hi], self.r1r.at[s, :, self.hi], 2, s, self.left),
            self.send(got.at[self.block(self.xr), self.hi], self.r1l.at[s, :, self.hi], 3, s, self.right),
            self.send(got.at[self.block(self.xl), self.lo], self.r1r.at[s, :, self.lo], 4, s, self.left),
        )

    def second(self, i):
        s = i % 2
        got = self.got.at[s]
        return (
            self.send(got.at[self.block(self.xr), self.lo], self.r2l.at[s], 5, s, self.right),
            self.send(got.at[self.block(self.xl), self.hi], self.r2r.at[s], 6, s, self.left),
        )

    def place(self, i, chip):
        return pl.ds(pl.multiple_of(i * self.m + self.c * 4 * self.r + chip * self.r, 16), self.r)

    def own(self, i):
        s = i % 2
        mine, here = self.mine.at[s], self.whole.at[self.place(i, self.x), :]
        return (
            self.send(mine, here, 7, s, self.right),
            self.send(mine, here, 8, s, self.left),
            self.send(mine, here, 9, s, self.twin),
        )

    def keep(self, i):
        s = i % 2
        return pltpu.make_async_copy(self.mine.at[s], self.whole.at[self.place(i, self.x), :], self.sems.at[0, s, 15])

    def onward(self, i):
        s = i % 2
        a, b = self.whole.at[self.place(i, self.xl), self.lo], self.whole.at[self.place(i, self.xr), self.hi]
        return self.send(a, a, 10, s, self.right), self.send(b, b, 11, s, self.left)

    def across(self, i):
        s = i % 2
        a, b = self.whole.at[self.place(i, self.xl), :], self.whole.at[self.place(i, self.xr), :]
        return self.send(a, a, 12, s, self.twin), self.send(b, b, 13, s, self.twin)

    def last(self, i):
        s = i % 2
        a = self.whole.at[self.place(i, self.xo), :]
        return self.send(a, a, 14, s, self.twin)


    def s0(self, i):
        self.pair(i).start()

    def s1(self, i):
        self.pair(i).wait()
        s, r = i % 2, self.r
        base = self.c * 4 * r

        def add(k, _):
            a = _rows(k, 16)
            b = pl.ds(pl.multiple_of(base + k * 16, 16), 16)
            self.got[s, a, :] = (self.got[s, a, :].astype(F32) + self.part[b, :].astype(F32)).astype(BF16)
            return 0

        lax.fori_loop(0, 4 * r // 16, add, 0)
        for copy in self.first(i):
            copy.start()

    def s2(self, i):
        s, r = i % 2, self.r
        copies = self.first(i)
        for copy in copies:
            copy.wait_send()
        copies[0].wait_recv()
        copies[1].wait_recv()

        def add(k, _):
            a = _rows(k, 16)
            for chip, cols, new in ((self.xr, self.lo, self.r1l), (self.xl, self.hi, self.r1r)):
                b = pl.ds(pl.multiple_of(chip * r + k * 16, 16), 16)
                self.got[s, b, cols] = (self.got[s, b, cols].astype(F32) + new[s, a, cols].astype(F32)).astype(BF16)
            return 0

        lax.fori_loop(0, r // 16, add, 0)
        for copy in self.second(i):
            copy.start()

    def s3(self, i):
        s, r = i % 2, self.r
        copies = self.first(i)
        copies[2].wait_recv()
        copies[3].wait_recv()
        for copy in self.second(i):
            copy.wait()

        def add(k, _):
            a = _rows(k, 16)
            b = pl.ds(pl.multiple_of(self.x * r + k * 16, 16), 16)
            got = self.got[s, b, :].astype(F32)
            lo = got[:, :self.h] + self.r2l[s, a, :].astype(F32) + self.r1r[s, a, self.lo].astype(F32)
            hi = got[:, self.h:] + self.r1l[s, a, self.hi].astype(F32) + self.r2r[s, a, :].astype(F32)
            total = jnp.concatenate([lo, hi], axis=1).astype(BF16)
            self.mine[s, a, :] = self.finish(i, a, total)
            return 0

        lax.fori_loop(0, r // 16, add, 0)
        for copy in self.own(i):
            copy.start()
        self.keep(i).start()

    def s4(self, i):
        copies = self.own(i)
        for copy in copies:
            copy.wait_send()
        copies[0].wait_recv()
        copies[1].wait_recv()
        for copy in self.onward(i):
            copy.start()
        for copy in self.across(i):
            copy.start()

    def s5(self, i):
        for copy in self.onward(i):
            copy.wait()
        self.last(i).start()

    def s6(self, i):
        self.own(i)[2].wait_recv()
        for copy in self.across(i):
            copy.wait()
        self.last(i).wait()
        self.keep(i).wait()


def _layer_kernel(m, o_hbm, x_hbm, g_ref, wo_hbm, wg_hbm, wu_hbm, wd_hbm, y_hbm, b_hbm,
                  wo_buf, o_buf, x_buf, h_buf, b_buf, u_buf, wgu_buf, wd_buf,
                  p_part, p_got, p_r1l, p_r1r, p_r2l, p_r2r, p_mine,
                  r_part, r_got, r_r1l, r_r1r, r_r2l, r_r2r, r_mine,
                  p_sems, r_sems, sems, wgu_sems, wd_sems):
    n, d = x_hbm.shape
    f = wg_hbm.shape[1]
    ft, dt = wgu_buf.shape[2] // 2, wd_buf.shape[2]
    nf, nd, nc = f // ft, d // dt, n // m
    r = m // 8

    def finish_p(i, a, total):
        xf = x_buf[a, :].astype(F32) + total.astype(F32)
        h = xf.astype(BF16)
        h_buf[i, a, :] = h
        hf = h.astype(F32)
        ms = jnp.mean(hf * hf, axis=-1, keepdims=True)
        return (hf * lax.rsqrt(ms + EPS) * g_ref[...].astype(F32)).astype(BF16)

    def finish_r(i, a, total):
        return (h_buf[i, a, :].astype(F32) + total.astype(F32)).astype(BF16)

    ps = _Stream(m, p_part, p_got, p_r1l, p_r1r, p_r2l, p_r2r, p_mine, b_hbm, p_sems, finish_p)
    rs = _Stream(m, r_part, r_got, r_r1l, r_r1r, r_r2l, r_r2r, r_mine, y_hbm, r_sems, finish_r)

    barrier = pltpu.get_barrier_semaphore()
    for to in (ps.right, ps.left, ps.twin):
        pl.semaphore_signal(barrier, inc=1, device_id={"tp": to}, device_id_type=pl.DeviceIdType.MESH)
    pl.semaphore_wait(barrier, 3)

    def wgu(k, s):
        c = _cols(k, ft)
        return (pltpu.make_async_copy(wg_hbm.at[:, c], wgu_buf.at[s, :, pl.ds(0, ft)], wgu_sems.at[s, 0]),
                pltpu.make_async_copy(wu_hbm.at[:, c], wgu_buf.at[s, :, pl.ds(ft, ft)], wgu_sems.at[s, 1]))

    def wd(k, s):
        return pltpu.make_async_copy(wd_hbm.at[:, _cols(k, dt)], wd_buf.at[s], wd_sems.at[s])

    def load_o(i):
        return pltpu.make_async_copy(o_hbm.at[_rows(i, m), :], o_buf, sems.at[0])

    def load_x(i):
        return pltpu.make_async_copy(x_hbm.at[ps.place(i, ps.x), :], x_buf, sems.at[1])

    def load_b(i):
        return pltpu.make_async_copy(b_hbm.at[_rows(i, m), :], b_buf, sems.at[2])

    load_wo = pltpu.make_async_copy(wo_hbm, wo_buf, sems.at[3])
    load_o(0).start()
    load_wo.start()
    for k in range(2):
        for copy in wgu(k % nf, k):
            copy.start()
        wd(k % nd, k).start()

    def gate_up(i, lo, hi):
        def tile(k, _):
            at = i * nf + k
            s = at % 2
            for copy in wgu(k, s):
                copy.wait()
            z = _dot(b_buf[...], wgu_buf[s])
            gate = z[:, :ft].astype(BF16).astype(F32)
            up = z[:, ft:].astype(BF16).astype(F32)
            u_buf[:, _cols(k, ft)] = (gate * (1.0 / (1.0 + jnp.exp(-gate))) * up).astype(BF16)

            @pl.when(at + 2 < nc * nf)
            def _():
                for copy in wgu((k + 2) % nf, s):
                    copy.start()
            return 0

        lax.fori_loop(lo, hi, tile, 0)

    def down(i, lo, hi):
        def tile(k, _):
            at = i * nd + k
            s = at % 2
            wd(k, s).wait()
            r_part[:, _cols(k, dt)] = _dot(u_buf[...], wd_buf[s]).astype(BF16)

            @pl.when(at + 2 < nc * nd)
            def _():
                wd((k + 2) % nd, s).start()
            return 0

        lax.fori_loop(lo, hi, tile, 0)

    def out_proj(i):
        load_o(i).wait()

        @pl.when(i == 0)
        def _():
            load_wo.wait()

        def tile(k, _):
            p_part[:, _cols(k, dt)] = _dot(o_buf[...], wo_buf[:, _cols(k, dt)]).astype(BF16)
            return 0

        lax.fori_loop(0, nd, tile, 0)

        @pl.when(i + 1 < nc)
        def _():
            load_o(i + 1).start()

    def step(j, _):
        def at(delay):
            return lambda body: pl.when((j >= delay) & (j < nc + delay))(lambda: body(j - delay))

        at(4)(rs.s4)
        at(3)(rs.s1)
        at(0)(out_proj)
        at(1)(ps.s3)
        at(0)(ps.s0)

        @at(2)
        def _(i):
            ps.s6(i)
            load_b(i).start()
            load_b(i).wait()
            gate_up(i, 0, (nf + 1) // 2)

        at(4)(rs.s5)
        at(3)(rs.s2)
        at(2)(lambda i: gate_up(i, (nf + 1) // 2, nf))
        at(1)(ps.s4)
        at(0)(ps.s1)
        at(2)(lambda i: down(i, 0, nd // 2))
        at(4)(rs.s6)
        at(3)(rs.s3)
        at(2)(lambda i: down(i, nd // 2, nd))
        at(1)(ps.s5)

        @at(0)
        def _(i):
            load_x(i).start()
            ps.s2(i)
            load_x(i).wait()

        at(2)(rs.s0)
        return 0

    lax.fori_loop(0, nc + 5, step, 0)


def _layer_sums(o, x, g2, wo, wg, wu, wd):
    n, d = x.shape
    m = _rows_per_chunk(n)
    r, h, hq, f = m // 8, d // 2, o.shape[1], wg.shape[1]
    ft, dt = 256, 512
    stream = [pltpu.VMEM((m, d), BF16), pltpu.VMEM((2, 4 * r, d), BF16),
              pltpu.VMEM((2, r, d), BF16), pltpu.VMEM((2, r, d), BF16),
              pltpu.VMEM((2, r, h), BF16), pltpu.VMEM((2, r, h), BF16), pltpu.VMEM((2, r, d), BF16)]
    return pl.pallas_call(
        functools.partial(_layer_kernel, m),
        out_shape=(jax.ShapeDtypeStruct((n, d), BF16), jax.ShapeDtypeStruct((n, d), BF16)),
        in_specs=[ANY, ANY, pl.BlockSpec(memory_space=pltpu.VMEM), ANY, ANY, ANY, ANY],
        out_specs=(ANY, ANY),
        scratch_shapes=[
            pltpu.VMEM((hq, d), BF16), pltpu.VMEM((m, hq), BF16), pltpu.VMEM((r, d), BF16),
            pltpu.VMEM((n // m, r, d), BF16), pltpu.VMEM((m, d), BF16), pltpu.VMEM((m, f), BF16),
            pltpu.VMEM((2, d, 2 * ft), BF16), pltpu.VMEM((2, f, dt), BF16),
            *stream, *stream,
            pltpu.SemaphoreType.DMA((2, 2, 16)), pltpu.SemaphoreType.DMA((2, 2, 16)),
            pltpu.SemaphoreType.DMA((4,)), pltpu.SemaphoreType.DMA((2, 2)), pltpu.SemaphoreType.DMA((2,)),
        ],
        compiler_params=pltpu.CompilerParams(collective_id=0, has_side_effects=True, vmem_limit_bytes=VMEM_LIMIT),
        name="layer_sums",
    )(o, x, g2, wo, wg, wu, wd)


def _cache_kernel(m, l1_ref, k_ref, v_ref, ck_ref, cv_ref, k_buf, v_buf):
    i = pl.program_id(0)
    n = k_ref.shape[0]
    l1 = l1_ref[0]

    @pl.when(i == 0)
    def _():
        for src, buf in ((k_ref, k_buf), (v_ref, v_buf)):
            buf[pl.ds(0, n), :] = src[...].astype(F32)
            buf[pl.ds(n, m), :] = jnp.zeros((m, HEAD), F32)

    rows = i * m + lax.broadcasted_iota(jnp.int32, (m, 1), 0)
    start = jnp.minimum(l1 + i * m, n)
    for buf, out in ((k_buf, ck_ref), (v_buf, cv_ref)):
        out[0] = jnp.where(rows < l1, buf[_rows(i, m), :], 0.0).astype(BF16)
        out[1] = jnp.where(rows < n - l1, buf[pl.ds(start, m), :], 0.0).astype(BF16)


def _caches(lens, k, v):
    n = k.shape[0]
    m = _rows_per_chunk(n)
    whole = pl.BlockSpec((n, HEAD), lambda i: (0, 0))
    out = pl.BlockSpec((2, m, HEAD), lambda i: (0, i, 0))
    return pl.pallas_call(
        functools.partial(_cache_kernel, m),
        grid=(n // m,),
        out_shape=(jax.ShapeDtypeStruct((2, n, HEAD), BF16),) * 2,
        in_specs=[pl.BlockSpec(memory_space=pltpu.SMEM), whole, whole],
        out_specs=(out, out),
        scratch_shapes=[pltpu.VMEM((n + m, HEAD), F32), pltpu.VMEM((n + m, HEAD), F32)],
        compiler_params=pltpu.CompilerParams(dimension_semantics=("arbitrary",)),
        name="caches",
    )(lens, k, v)


def solution(mesh):
    assert mesh.shape["tp"] == 8

    def layer(x, lens, g1, g2, wq, wk, wv, wo, wg, wu, wd):
        n, d = x.shape
        t = lax.axis_index("tp")
        l1 = lens[0]
        rows = jnp.arange(n)
        pos = jnp.where(rows >= l1, rows - l1, rows)
        inv = BASE ** (-jnp.arange(0, HEAD, 2, dtype=F32) / HEAD)
        ang = pos.astype(F32)[:, None] * inv[None, :]
        c, s = jnp.cos(ang), jnp.sin(ang)
        cos = jnp.concatenate([c, c], axis=1)
        sin = jnp.concatenate([-s, s], axis=1)
        wkv = jnp.concatenate([lax.dynamic_slice_in_dim(w, t * HEAD, HEAD, axis=1) for w in (wk, wv)], axis=1)
        o, k, v = _attention(x, lens, g1[None], cos, sin, wq, wkv)
        y, _ = _layer_sums(o, x, g2[None], wo, wg, wu, wd)
        ck, cv = _caches(lens, k, v)
        return y, ck[:, :, None, :], cv[:, :, None, :]

    row = P("dp", None)
    cache = P("dp", None, "tp", None)
    return jax.shard_map(
        layer, mesh=mesh,
        in_specs=(row, P("dp"), P(), P(), P(None, "tp"), P(), P(), P("tp", None),
                  P(None, "tp"), P(None, "tp"), P("tp", None)),
        out_specs=(row, cache, cache), check_vma=False)
```

```python
import functools

import jax
import jax.numpy as jnp
from jax import lax
from jax.experimental import pallas as pl
from jax.experimental.pallas import tpu as pltpu
from jax.sharding import PartitionSpec as P

HEAD = 128
EPS = 1e-5
BASE = 500000.0
VMEM_LIMIT = 67000000
F32 = jnp.float32
BF16 = jnp.bfloat16
ANY = pl.BlockSpec(memory_space=pl.ANY)


def _rows_per_chunk(n):
    return 384 if n % 384 == 0 else 128


def _dot(a, b):
    return jnp.dot(a, b, preferred_element_type=F32)


def _cols(i, size):
    return pl.ds(pl.multiple_of(i * size, size), size)


def _rows(i, size):
    return pl.ds(pl.multiple_of(i * size, size), size)


def _norm_chunk(m, x_ref, g, a_ref):
    def body(k, _):
        r = _rows(k, 16)
        xf = x_ref[r, :].astype(F32)
        ms = jnp.mean(xf * xf, axis=-1, keepdims=True)
        a_ref[r, :] = (xf * lax.rsqrt(ms + EPS) * g).astype(BF16)
        return 0

    lax.fori_loop(0, m // 16, body, 0)


def _rope(z, cos, sin):
    return z * cos + pltpu.roll(z, HEAD // 2, 1) * sin


def _project_chunk(i, m, a_ref, wq_ref, wkv_ref, cos_ref, sin_ref, q_ref, k_ref, v_ref):
    a = a_ref[...]
    cos, sin = cos_ref[...], sin_ref[...]
    kv = _dot(a, wkv_ref[...])
    r = _rows(i, m)
    k_ref[r, :] = _rope(kv[:, :HEAD], cos, sin).astype(BF16)
    v_ref[r, :] = kv[:, HEAD:].astype(BF16)
    q = _dot(a, wq_ref[...])
    for h in range(q_ref.shape[0]):
        q_ref[h] = _rope(q[:, h * HEAD:(h + 1) * HEAD], cos, sin).astype(BF16)


def _attend_chunk(i, m, l1, q_ref, k_ref, v_ref, s_ref, o_ref):
    rows = i * m + lax.broadcasted_iota(jnp.int32, (m, 1), 0)
    first = jnp.where(rows >= l1, l1, 0)
    scale = HEAD ** -0.5 * 1.4426950408889634

    def head(h, _):
        q = q_ref[h]

        def score(b, top):
            s = lax.dot_general(q, k_ref[_rows(b, m), :], (((1,), (1,)), ((), ())), preferred_element_type=F32)
            cols = b * m + lax.broadcasted_iota(jnp.int32, (1, m), 1)
            s = jnp.where((cols <= rows) & (cols >= first), s, -jnp.inf)
            s_ref[b] = s
            return jnp.maximum(top, jnp.max(s, axis=1, keepdims=True))

        top = lax.fori_loop(0, i + 1, score, jnp.full((m, 1), -jnp.inf, F32))

        def expo(b, total):
            e = jnp.exp2((s_ref[b] - top) * scale)
            s_ref[b] = e
            return total + jnp.sum(e, axis=1, keepdims=True)

        total = lax.fori_loop(0, i + 1, expo, jnp.zeros((m, 1), F32))
        inv = 1.0 / total

        def value(b, acc):
            return acc + _dot((s_ref[b] * inv).astype(BF16), v_ref[_rows(b, m), :])

        acc = lax.fori_loop(0, i + 1, value, jnp.zeros((m, HEAD), F32))
        o_ref[:, _cols(h, HEAD)] = acc.astype(BF16)
        return 0

    lax.fori_loop(0, q_ref.shape[0], head, 0)


class _Stream:
    def __init__(self, m, part, got, r1l, r1r, r2l, r2r, mine, whole, sems, finish):
        self.m, self.r = m, m // 8
        self.part, self.got, self.mine, self.whole = part, got, mine, whole
        self.r1l, self.r1r, self.r2l, self.r2r = r1l, r1r, r2l, r2r
        self.sems, self.finish = sems, finish
        self.h = part.shape[1] // 2
        t = lax.axis_index("tp")
        x, c = t // 2, t % 2
        self.x, self.c = x, c
        self.xr, self.xo, self.xl = (x + 1) % 4, (x + 2) % 4, (x + 3) % 4
        self.right, self.left = self.xr * 2 + c, self.xl * 2 + c
        self.twin = x * 2 + 1 - c
        self.lo, self.hi = pl.ds(0, self.h), pl.ds(self.h, self.h)

    def send(self, src, dst, k, slot, to):
        return pltpu.make_async_remote_copy(
            src_ref=src, dst_ref=dst, send_sem=self.sems.at[0, slot, k], recv_sem=self.sems.at[1, slot, k],
            device_id={"tp": to}, device_id_type=pl.DeviceIdType.MESH)

    def block(self, chip):
        return pl.ds(pl.multiple_of(chip * self.r, 16), self.r)

    def pair(self, i):
        s = i % 2
        theirs = pl.ds(pl.multiple_of((1 - self.c) * 4 * self.r, 16), 4 * self.r)
        return self.send(self.part.at[theirs, :], self.got.at[s], 0, s, self.twin)

    def first(self, i):
        s = i % 2
        got = self.got.at[s]
        return (
            self.send(got.at[self.block(self.xo), self.lo], self.r1l.at[s, :, self.lo], 1, s, self.right),
            self.send(got.at[self.block(self.xo), self.hi], self.r1r.at[s, :, self.hi], 2, s, self.left),
            self.send(got.at[self.block(self.xr), self.hi], self.r1l.at[s, :, self.hi], 3, s, self.right),
            self.send(got.at[self.block(self.xl), self.lo], self.r1r.at[s, :, self.lo], 4, s, self.left),
        )

    def second(self, i):
        s = i % 2
        got = self.got.at[s]
        return (
            self.send(got.at[self.block(self.xr), self.lo], self.r2l.at[s], 5, s, self.right),
            self.send(got.at[self.block(self.xl), self.hi], self.r2r.at[s], 6, s, self.left),
        )

    def place(self, i, chip):
        return pl.ds(pl.multiple_of(i * self.m + self.c * 4 * self.r + chip * self.r, 16), self.r)

    def own(self, i):
        s = i % 2
        mine, here = self.mine.at[s], self.whole.at[self.place(i, self.x), :]
        return (
            self.send(mine, here, 7, s, self.right),
            self.send(mine, here, 8, s, self.left),
            self.send(mine, here, 9, s, self.twin),
        )

    def keep(self, i):
        s = i % 2
        return pltpu.make_async_copy(self.mine.at[s], self.whole.at[self.place(i, self.x), :], self.sems.at[0, s, 15])

    def onward(self, i):
        s = i % 2
        a, b = self.whole.at[self.place(i, self.xl), self.lo], self.whole.at[self.place(i, self.xr), self.hi]
        return self.send(a, a, 10, s, self.right), self.send(b, b, 11, s, self.left)

    def across(self, i):
        s = i % 2
        a, b = self.whole.at[self.place(i, self.xl), :], self.whole.at[self.place(i, self.xr), :]
        return self.send(a, a, 12, s, self.twin), self.send(b, b, 13, s, self.twin)

    def last(self, i):
        s = i % 2
        a = self.whole.at[self.place(i, self.xo), :]
        return self.send(a, a, 14, s, self.twin)


    def s0(self, i):
        self.pair(i).start()

    def s1(self, i):
        self.pair(i).wait()
        s, r = i % 2, self.r
        base = self.c * 4 * r

        def add(k, _):
            a = _rows(k, 16)
            b = pl.ds(pl.multiple_of(base + k * 16, 16), 16)
            self.got[s, a, :] = (self.got[s, a, :].astype(F32) + self.part[b, :].astype(F32)).astype(BF16)
            return 0

        lax.fori_loop(0, 4 * r // 16, add, 0)
        for copy in self.first(i):
            copy.start()

    def s2(self, i):
        s, r = i % 2, self.r
        copies = self.first(i)
        for copy in copies:
            copy.wait_send()
        copies[0].wait_recv()
        copies[1].wait_recv()

        def add(k, _):
            a = _rows(k, 16)
            for chip, cols, new in ((self.xr, self.lo, self.r1l), (self.xl, self.hi, self.r1r)):
                b = pl.ds(pl.multiple_of(chip * r + k * 16, 16), 16)
                self.got[s, b, cols] = (self.got[s, b, cols].astype(F32) + new[s, a, cols].astype(F32)).astype(BF16)
            return 0

        lax.fori_loop(0, r // 16, add, 0)
        for copy in self.second(i):
            copy.start()

    def s3(self, i):
        s, r = i % 2, self.r
        copies = self.first(i)
        copies[2].wait_recv()
        copies[3].wait_recv()
        for copy in self.second(i):
            copy.wait()

        def add(k, _):
            a = _rows(k, 16)
            b = pl.ds(pl.multiple_of(self.x * r + k * 16, 16), 16)
            got = self.got[s, b, :].astype(F32)
            lo = got[:, :self.h] + self.r2l[s, a, :].astype(F32) + self.r1r[s, a, self.lo].astype(F32)
            hi = got[:, self.h:] + self.r1l[s, a, self.hi].astype(F32) + self.r2r[s, a, :].astype(F32)
            total = jnp.concatenate([lo, hi], axis=1).astype(BF16)
            self.mine[s, a, :] = self.finish(i, a, total)
            return 0

        lax.fori_loop(0, r // 16, add, 0)
        for copy in self.own(i):
            copy.start()
        self.keep(i).start()

    def s4(self, i):
        copies = self.own(i)
        for copy in copies:
            copy.wait_send()
        copies[0].wait_recv()
        copies[1].wait_recv()
        for copy in self.onward(i):
            copy.start()
        for copy in self.across(i):
            copy.start()

    def s5(self, i):
        for copy in self.onward(i):
            copy.wait()
        self.last(i).start()

    def s6(self, i):
        self.own(i)[2].wait_recv()
        for copy in self.across(i):
            copy.wait()
        self.last(i).wait()
        self.keep(i).wait()


def _layer_kernel(m, l1_ref, x_hbm, g1_ref, g2_ref, cos_hbm, sin_hbm, wq_hbm, wk_hbm, wv_hbm, wo_hbm, wg_hbm, wu_hbm, wd_hbm,
                  y_hbm, b_hbm, k_hbm, v_hbm,
                  wq_buf, wkv_buf, wo_buf, cos_buf, sin_buf, q_buf, k_buf, v_buf, s_buf, o_buf,
                  x_buf, h_buf, xb_buf, u_buf, wgu_buf, wd_buf,
                  p_part, p_got, p_r1l, p_r1r, p_r2l, p_r2r, p_mine,
                  r_part, r_got, r_r1l, r_r1r, r_r2l, r_r2r, r_mine,
                  p_sems, r_sems, sems, wgu_sems, wd_sems):
    n, d = x_hbm.shape
    f = wg_hbm.shape[1]
    ft, dt = wgu_buf.shape[2] // 2, wd_buf.shape[2]
    nf, nd, nc = f // ft, d // dt, n // m
    r = m // 8

    def finish_p(i, a, total):
        xf = x_buf[a, :].astype(F32) + total.astype(F32)
        h = xf.astype(BF16)
        h_buf[i, a, :] = h
        hf = h.astype(F32)
        ms = jnp.mean(hf * hf, axis=-1, keepdims=True)
        return (hf * lax.rsqrt(ms + EPS) * g2_ref[...].astype(F32)).astype(BF16)

    def finish_r(i, a, total):
        return (h_buf[i, a, :].astype(F32) + total.astype(F32)).astype(BF16)

    ps = _Stream(m, p_part, p_got, p_r1l, p_r1r, p_r2l, p_r2r, p_mine, b_hbm, p_sems, finish_p)
    rs = _Stream(m, r_part, r_got, r_r1l, r_r1r, r_r2l, r_r2r, r_mine, y_hbm, r_sems, finish_r)

    barrier = pltpu.get_barrier_semaphore()
    for to in (ps.right, ps.left, ps.twin):
        pl.semaphore_signal(barrier, inc=1, device_id={"tp": to}, device_id_type=pl.DeviceIdType.MESH)
    pl.semaphore_wait(barrier, 3)

    def wgu(k, s):
        c = _cols(k, ft)
        return (pltpu.make_async_copy(wg_hbm.at[:, c], wgu_buf.at[s, :, pl.ds(0, ft)], wgu_sems.at[s, 0]),
                pltpu.make_async_copy(wu_hbm.at[:, c], wgu_buf.at[s, :, pl.ds(ft, ft)], wgu_sems.at[s, 1]))

    def wd(k, s):
        return pltpu.make_async_copy(wd_hbm.at[:, _cols(k, dt)], wd_buf.at[s], wd_sems.at[s])

    def load_chunk(i):
        r = _rows(i, m)
        return (pltpu.make_async_copy(x_hbm.at[r, :], xb_buf, sems.at[0]),
                pltpu.make_async_copy(cos_hbm.at[r, :], cos_buf, sems.at[4]),
                pltpu.make_async_copy(sin_hbm.at[r, :], sin_buf, sems.at[5]))

    def store_kv(i):
        r = _rows(i, m)
        return (pltpu.make_async_copy(k_buf.at[r, :], k_hbm.at[r, :], sems.at[6]),
                pltpu.make_async_copy(v_buf.at[r, :], v_hbm.at[r, :], sems.at[7]))

    def load_x(i):
        return pltpu.make_async_copy(x_hbm.at[ps.place(i, ps.x), :], x_buf, sems.at[1])

    def load_b(i):
        return pltpu.make_async_copy(b_hbm.at[_rows(i, m), :], xb_buf, sems.at[2])

    head = _cols(lax.axis_index("tp"), HEAD)
    load_wo = pltpu.make_async_copy(wo_hbm, wo_buf, sems.at[3])
    load_qkv = (pltpu.make_async_copy(wk_hbm.at[:, head], wkv_buf.at[:, pl.ds(0, HEAD)], sems.at[8]),
                pltpu.make_async_copy(wv_hbm.at[:, head], wkv_buf.at[:, pl.ds(HEAD, HEAD)], sems.at[9]),
                pltpu.make_async_copy(wq_hbm, wq_buf, sems.at[10]))
    for copy in (*load_chunk(0), *load_qkv, load_wo):
        copy.start()
    for k in range(2):
        for copy in wgu(k % nf, k):
            copy.start()
        wd(k % nd, k).start()

    def gate_up(i, lo, hi):
        def tile(k, _):
            at = i * nf + k
            s = at % 2
            for copy in wgu(k, s):
                copy.wait()
            z = _dot(xb_buf[...], wgu_buf[s])
            gate = z[:, :ft].astype(BF16).astype(F32)
            up = z[:, ft:].astype(BF16).astype(F32)
            u_buf[:, _cols(k, ft)] = (gate * (1.0 / (1.0 + jnp.exp(-gate))) * up).astype(BF16)

            @pl.when(at + 2 < nc * nf)
            def _():
                for copy in wgu((k + 2) % nf, s):
                    copy.start()
            return 0

        lax.fori_loop(lo, hi, tile, 0)

    def down(i, lo, hi):
        def tile(k, _):
            at = i * nd + k
            s = at % 2
            wd(k, s).wait()
            r_part[:, _cols(k, dt)] = _dot(u_buf[...], wd_buf[s]).astype(BF16)

            @pl.when(at + 2 < nc * nd)
            def _():
                wd((k + 2) % nd, s).start()
            return 0

        lax.fori_loop(lo, hi, tile, 0)

    def project(i):
        for copy in load_chunk(i):
            copy.wait()
        _norm_chunk(m, xb_buf, g1_ref[...].astype(F32), xb_buf)

        @pl.when(i == 0)
        def _():
            for copy in load_qkv:
                copy.wait()

        _project_chunk(i, m, xb_buf, wq_buf, wkv_buf, cos_buf, sin_buf, q_buf, k_buf, v_buf)
        for copy in store_kv(i):
            copy.start()

    def attend(i):
        _attend_chunk(i, m, l1_ref[0], q_buf, k_buf, v_buf, s_buf, o_buf)

        @pl.when(i == 0)
        def _():
            load_wo.wait()

        def tile(k, _):
            p_part[:, _cols(k, dt)] = _dot(o_buf[...], wo_buf[:, _cols(k, dt)]).astype(BF16)
            return 0

        lax.fori_loop(0, nd, tile, 0)
        for copy in store_kv(i):
            copy.wait()

    def step(j, _):
        def at(delay):
            return lambda body: pl.when((j >= delay) & (j < nc + delay))(lambda: body(j - delay))

        at(0)(project)
        at(4)(rs.s4)
        at(3)(rs.s1)
        at(0)(attend)
        at(1)(ps.s3)
        at(0)(ps.s0)

        @at(2)
        def _(i):
            ps.s6(i)
            load_b(i).start()
            load_b(i).wait()
            gate_up(i, 0, (nf + 1) // 2)

        at(4)(rs.s5)
        at(3)(rs.s2)
        at(2)(lambda i: gate_up(i, (nf + 1) // 2, nf))

        @pl.when(j + 1 < nc)
        def _():
            for copy in load_chunk(j + 1):
                copy.start()

        at(1)(ps.s4)
        at(0)(ps.s1)
        at(2)(lambda i: down(i, 0, nd // 2))
        at(4)(rs.s6)
        at(3)(rs.s3)
        at(2)(lambda i: down(i, nd // 2, nd))
        at(1)(ps.s5)

        @at(0)
        def _(i):
            load_x(i).start()
            ps.s2(i)
            load_x(i).wait()

        at(2)(rs.s0)
        return 0

    lax.fori_loop(0, nc + 5, step, 0)


def _layer(x, lens, g1, g2, cos, sin, wq, wk, wv, wo, wg, wu, wd):
    n, d = x.shape
    m = _rows_per_chunk(n)
    r, h, hq, f = m // 8, d // 2, wq.shape[1], wg.shape[1]
    ft, dt = 256, 512
    stream = [pltpu.VMEM((m, d), BF16), pltpu.VMEM((2, 4 * r, d), BF16),
              pltpu.VMEM((2, r, d), BF16), pltpu.VMEM((2, r, d), BF16),
              pltpu.VMEM((2, r, h), BF16), pltpu.VMEM((2, r, h), BF16), pltpu.VMEM((2, r, d), BF16)]
    whole, head = jax.ShapeDtypeStruct((n, d), BF16), jax.ShapeDtypeStruct((n, HEAD), BF16)
    vmem = pl.BlockSpec(memory_space=pltpu.VMEM)
    return pl.pallas_call(
        functools.partial(_layer_kernel, m),
        out_shape=(whole, whole, head, head),
        in_specs=[pl.BlockSpec(memory_space=pltpu.SMEM), ANY, vmem, vmem] + [ANY] * 9,
        out_specs=(ANY,) * 4,
        scratch_shapes=[
            pltpu.VMEM((d, hq), BF16), pltpu.VMEM((d, 2 * HEAD), BF16), pltpu.VMEM((hq, d), BF16),
            pltpu.VMEM((m, HEAD), F32), pltpu.VMEM((m, HEAD), F32), pltpu.VMEM((hq // HEAD, m, HEAD), BF16),
            pltpu.VMEM((n, HEAD), BF16), pltpu.VMEM((n, HEAD), BF16), pltpu.VMEM((n // m, m, m), F32),
            pltpu.VMEM((m, hq), BF16),
            pltpu.VMEM((r, d), BF16), pltpu.VMEM((n // m, r, d), BF16), pltpu.VMEM((m, d), BF16),
            pltpu.VMEM((m, f), BF16), pltpu.VMEM((2, d, 2 * ft), BF16), pltpu.VMEM((2, f, dt), BF16),
            *stream, *stream,
            pltpu.SemaphoreType.DMA((2, 2, 16)), pltpu.SemaphoreType.DMA((2, 2, 16)),
            pltpu.SemaphoreType.DMA((11,)), pltpu.SemaphoreType.DMA((2, 2)), pltpu.SemaphoreType.DMA((2,)),
        ],
        compiler_params=pltpu.CompilerParams(collective_id=0, has_side_effects=True, vmem_limit_bytes=VMEM_LIMIT),
        name="layer",
    )(lens, x, g1, g2, cos, sin, wq, wk, wv, wo, wg, wu, wd)


def _finish_kernel(m, l1_ref, y_in, k_in, v_in, y_out, ck_out, cv_out, y_buf, k_buf, v_buf, kf_buf, vf_buf, ck_buf, cv_buf,
                   in_sems, out_sems, sems):
    n = y_in.shape[0]
    nc = n // m
    l1 = l1_ref[0]
    rows = [pl.ds(i * m, m) for i in range(nc)]
    loads = [pltpu.make_async_copy(y_in.at[rows[i], :], y_buf.at[i], in_sems.at[i]) for i in range(nc)]
    stores = [pltpu.make_async_copy(y_buf.at[i], y_out.at[rows[i], :], out_sems.at[i]) for i in range(nc)]
    heads = [pltpu.make_async_copy(k_in, k_buf, sems.at[0]), pltpu.make_async_copy(v_in, v_buf, sems.at[1])]
    caches = [pltpu.make_async_copy(ck_buf, ck_out, sems.at[2]), pltpu.make_async_copy(cv_buf, cv_out, sems.at[3])]
    for copy in heads + loads:
        copy.start()
    for copy in heads:
        copy.wait()
    for src, buf in ((k_buf, kf_buf), (v_buf, vf_buf)):
        buf[pl.ds(n, m), :] = jnp.zeros((m, HEAD), F32)

        def widen(i, _):
            buf[_rows(i, m), :] = src[_rows(i, m), :].astype(F32)
            return 0

        lax.fori_loop(0, nc, widen, 0)
    for i in range(nc):
        loads[i].wait()
        stores[i].start()
        at = i * m + lax.broadcasted_iota(jnp.int32, (m, 1), 0)
        start = jnp.minimum(l1 + i * m, n)
        for buf, out in ((kf_buf, ck_buf), (vf_buf, cv_buf)):
            out[0, rows[i], :] = jnp.where(at < l1, buf[rows[i], :], 0.0).astype(BF16)
            out[1, rows[i], :] = jnp.where(at < n - l1, buf[pl.ds(start, m), :], 0.0).astype(BF16)
    for copy in caches:
        copy.start()
    for copy in caches + stores:
        copy.wait()


def _finish(lens, y, k, v):
    n, d = y.shape
    m = _rows_per_chunk(n)
    cache = jax.ShapeDtypeStruct((2, n, HEAD), BF16)
    return pl.pallas_call(
        functools.partial(_finish_kernel, m),
        out_shape=(jax.ShapeDtypeStruct((n, d), BF16), cache, cache),
        in_specs=[pl.BlockSpec(memory_space=pltpu.SMEM), ANY, ANY, ANY],
        out_specs=(ANY,) * 3,
        scratch_shapes=[pltpu.VMEM((n // m, m, d), BF16), pltpu.VMEM((n, HEAD), BF16), pltpu.VMEM((n, HEAD), BF16),
                        pltpu.VMEM((n + m, HEAD), F32), pltpu.VMEM((n + m, HEAD), F32),
                        pltpu.VMEM((2, n, HEAD), BF16), pltpu.VMEM((2, n, HEAD), BF16),
                        pltpu.SemaphoreType.DMA((n // m,)), pltpu.SemaphoreType.DMA((n // m,)), pltpu.SemaphoreType.DMA((4,))],
        compiler_params=pltpu.CompilerParams(vmem_limit_bytes=VMEM_LIMIT),
        name="finish",
    )(lens, y, k, v)


def solution(mesh):
    assert mesh.shape["tp"] == 8

    def layer(x, lens, g1, g2, wq, wk, wv, wo, wg, wu, wd):
        n, d = x.shape
        l1 = lens[0]
        rows = jnp.arange(n)
        pos = jnp.where(rows >= l1, rows - l1, rows)
        inv = BASE ** (-jnp.arange(0, HEAD, 2, dtype=F32) / HEAD)
        ang = pos.astype(F32)[:, None] * inv[None, :]
        c, s = jnp.cos(ang), jnp.sin(ang)
        cos = jnp.concatenate([c, c], axis=1)
        sin = jnp.concatenate([-s, s], axis=1)
        y, _, k, v = _layer(x, lens, g1[None], g2[None], cos, sin, wq, wk, wv, wo, wg, wu, wd)
        y, ck, cv = _finish(lens, y, k, v)
        return y, ck[:, :, None, :], cv[:, :, None, :]

    row = P("dp", None)
    cache = P("dp", None, "tp", None)
    return jax.shard_map(
        layer, mesh=mesh,
        in_specs=(row, P("dp"), P(), P(), P(None, "tp"), P(), P(), P("tp", None),
                  P(None, "tp"), P(None, "tp"), P("tp", None)),
        out_specs=(row, cache, cache), check_vma=False)
```

```python
import functools

import jax
import jax.numpy as jnp
from jax import lax
from jax.experimental import pallas as pl
from jax.experimental.pallas import tpu as pltpu
from jax.sharding import PartitionSpec as P

HEAD = 128
EPS = 1e-5
BASE = 500000.0
VMEM_LIMIT = 67000000
F32 = jnp.float32
BF16 = jnp.bfloat16
ANY = pl.BlockSpec(memory_space=pl.ANY)


def _rows_per_chunk(n):
    return 384 if n % 384 == 0 else 128


def _dot(a, b):
    return jnp.dot(a, b, preferred_element_type=F32)


def _cols(i, size):
    return pl.ds(pl.multiple_of(i * size, size), size)


def _rows(i, size):
    return pl.ds(pl.multiple_of(i * size, size), size)


def _norm_chunk(m, x_ref, g, a_ref):
    step = 32

    def body(k, _):
        r = _rows(k, step)
        xf = x_ref[r, :].astype(F32)
        ms = jnp.mean(xf * xf, axis=-1, keepdims=True)
        a_ref[r, :] = (xf * lax.rsqrt(ms + EPS) * g).astype(BF16)
        return 0

    lax.fori_loop(0, m // step, body, 0)


def _project_chunk(i, m, second, a_ref, wq_ref, wkv_ref, cos_ref, sin_ref, q_ref, k_ref, v_ref, vt_ref):
    a = a_ref[...]
    low = lax.broadcasted_iota(jnp.int32, (m, HEAD), 1) < HEAD // 2
    mine = low != (second > 0)
    cos, sin = cos_ref[...], sin_ref[...]
    cos = jnp.where(mine, cos, pltpu.roll(cos, HEAD // 2, 1))
    sin = jnp.where(mine, sin, pltpu.roll(sin, HEAD // 2, 1))
    sin = jnp.where(low, -sin, sin)

    def rope(z):
        return (z * cos + pltpu.roll(z, HEAD // 2, 1) * sin).astype(BF16)

    kv = _dot(a, wkv_ref[...])
    k_ref[_rows(i, m), :] = rope(kv[:, :HEAD])
    v = kv[:, HEAD:]
    v_ref[...] = v.astype(BF16)
    vt_ref[:, _cols(i, m)] = v.T.astype(BF16)
    q = _dot(a, wq_ref[...])
    for h in range(q.shape[1] // HEAD):
        q_ref[pl.ds(h * m, m), :] = rope(q[:, h * HEAD:(h + 1) * HEAD])


def _attend_heads(i, m, l1, h0, heads, q_ref, k_ref, vt_ref, s_ref, acc_ref, o_ref):
    w = heads * m
    q = q_ref[pl.ds(h0 * m, w), :]
    rows = lax.broadcasted_iota(jnp.int32, (1, w), 1)
    for _ in range(heads - 1):
        rows = jnp.where(rows >= m, rows - m, rows)
    rows = rows + i * m
    first = jnp.where(rows >= l1, l1, 0)
    scale = HEAD ** -0.5 * 1.4426950408889634

    def scores(b):
        return lax.dot_general(k_ref[_rows(b, m), :], q, (((1,), (1,)), ((), ())), preferred_element_type=F32)

    def keys(b):
        return b * m + lax.broadcasted_iota(jnp.int32, (m, 1), 0)

    def take(b, top, total, new):
        peak = jnp.maximum(top, new)
        alpha = jnp.exp2((top - peak) * scale)
        e = jnp.exp2((s_ref[...] - peak) * scale)
        total = total * alpha + jnp.sum(e, axis=0, keepdims=True)
        acc_ref[...] = acc_ref[...] * alpha + _dot(vt_ref[:, _cols(b, m)], e.astype(BF16))
        return peak, total

    def put(s):
        s_ref[...] = s
        return jnp.max(s, axis=0, keepdims=True)

    acc_ref[...] = jnp.zeros_like(acc_ref)
    s = scores(i)
    new = put(jnp.where((keys(i) <= rows) & (keys(i) >= first), s, -jnp.inf))
    top, total = jnp.full((1, w), -jnp.inf, F32), jnp.zeros((1, w), F32)

    def block(b, carry):
        top, total, new = carry
        s = scores(b)
        top, total = take(jnp.where(b == 0, i, b - 1), top, total, new)
        return top, total, put(jnp.where(keys(b) >= first, s, -jnp.inf))

    top, total, new = lax.fori_loop(0, i, block, (top, total, new))
    top, total = take(jnp.where(i == 0, i, i - 1), top, total, new)
    o = acc_ref[...] * (1.0 / total)
    for h in range(heads):
        o_ref[:, pl.ds((h0 + h) * HEAD, HEAD)] = o[:, h * m:(h + 1) * m].T.astype(BF16)


class _Stream:
    def __init__(self, m, part, got, r1l, r1r, r2l, r2r, mine, whole, sems, finish):
        self.m, self.r = m, m // 8
        self.part, self.got, self.mine, self.whole = part, got, mine, whole
        self.r1l, self.r1r, self.r2l, self.r2r = r1l, r1r, r2l, r2r
        self.sems, self.finish = sems, finish
        self.h = part.shape[1] // 2
        t = lax.axis_index("tp")
        x, c = t // 2, t % 2
        self.x, self.c = x, c
        self.xr, self.xo, self.xl = (x + 1) % 4, (x + 2) % 4, (x + 3) % 4
        self.right, self.left = self.xr * 2 + c, self.xl * 2 + c
        self.twin = x * 2 + 1 - c
        self.lo, self.hi = pl.ds(0, self.h), pl.ds(self.h, self.h)

    def send(self, src, dst, k, slot, to):
        return pltpu.make_async_remote_copy(
            src_ref=src, dst_ref=dst, send_sem=self.sems.at[0, slot, k], recv_sem=self.sems.at[1, slot, k],
            device_id={"tp": to}, device_id_type=pl.DeviceIdType.MESH)

    def block(self, chip):
        return pl.ds(pl.multiple_of(chip * self.r, 16), self.r)

    def pair(self, i):
        s = i % 2
        theirs = pl.ds(pl.multiple_of((1 - self.c) * 4 * self.r, 16), 4 * self.r)
        return self.send(self.part.at[theirs, :], self.got.at[s], 0, s, self.twin)

    def first(self, i):
        s = i % 2
        got = self.got.at[s]
        return (
            self.send(got.at[self.block(self.xo), self.lo], self.r1l.at[s, :, self.lo], 1, s, self.right),
            self.send(got.at[self.block(self.xo), self.hi], self.r1r.at[s, :, self.hi], 2, s, self.left),
            self.send(got.at[self.block(self.xr), self.hi], self.r1l.at[s, :, self.hi], 3, s, self.right),
            self.send(got.at[self.block(self.xl), self.lo], self.r1r.at[s, :, self.lo], 4, s, self.left),
        )

    def second(self, i):
        s = i % 2
        got = self.got.at[s]
        return (
            self.send(got.at[self.block(self.xr), self.lo], self.r2l.at[s], 5, s, self.right),
            self.send(got.at[self.block(self.xl), self.hi], self.r2r.at[s], 6, s, self.left),
        )

    def place(self, i, chip):
        return pl.ds(pl.multiple_of(i * self.m + self.c * 4 * self.r + chip * self.r, 16), self.r)

    def own(self, i):
        s = i % 2
        mine, here = self.mine.at[s], self.whole.at[self.place(i, self.x), :]
        return (
            self.send(mine, here, 7, s, self.right),
            self.send(mine, here, 8, s, self.left),
            self.send(mine, here, 9, s, self.twin),
        )

    def keep(self, i):
        s = i % 2
        return pltpu.make_async_copy(self.mine.at[s], self.whole.at[self.place(i, self.x), :], self.sems.at[0, s, 15])

    def onward(self, i):
        s = i % 2
        a, b = self.whole.at[self.place(i, self.xl), self.lo], self.whole.at[self.place(i, self.xr), self.hi]
        return self.send(a, a, 10, s, self.right), self.send(b, b, 11, s, self.left)

    def across(self, i):
        s = i % 2
        a, b = self.whole.at[self.place(i, self.xl), :], self.whole.at[self.place(i, self.xr), :]
        return self.send(a, a, 12, s, self.twin), self.send(b, b, 13, s, self.twin)

    def last(self, i):
        s = i % 2
        a = self.whole.at[self.place(i, self.xo), :]
        return self.send(a, a, 14, s, self.twin)


    def s0(self, i):
        self.pair(i).start()

    def s1(self, i):
        self.pair(i).wait()
        s, r = i % 2, self.r
        base = self.c * 4 * r

        def add(k, _):
            a = _rows(k, 16)
            b = pl.ds(pl.multiple_of(base + k * 16, 16), 16)
            self.got[s, a, :] = (self.got[s, a, :].astype(F32) + self.part[b, :].astype(F32)).astype(BF16)
            return 0

        lax.fori_loop(0, 4 * r // 16, add, 0)
        for copy in self.first(i):
            copy.start()

    def s2(self, i):
        s, r = i % 2, self.r
        copies = self.first(i)
        for copy in copies:
            copy.wait_send()
        copies[0].wait_recv()
        copies[1].wait_recv()

        def add(k, _):
            a = _rows(k, 16)
            for chip, cols, new in ((self.xr, self.lo, self.r1l), (self.xl, self.hi, self.r1r)):
                b = pl.ds(pl.multiple_of(chip * r + k * 16, 16), 16)
                self.got[s, b, cols] = (self.got[s, b, cols].astype(F32) + new[s, a, cols].astype(F32)).astype(BF16)
            return 0

        lax.fori_loop(0, r // 16, add, 0)
        for copy in self.second(i):
            copy.start()

    def s3(self, i):
        s, r = i % 2, self.r
        copies = self.first(i)
        copies[2].wait_recv()
        copies[3].wait_recv()
        for copy in self.second(i):
            copy.wait()

        def add(k, _):
            a = _rows(k, 16)
            b = pl.ds(pl.multiple_of(self.x * r + k * 16, 16), 16)
            got = self.got[s, b, :].astype(F32)
            lo = got[:, :self.h] + self.r2l[s, a, :].astype(F32) + self.r1r[s, a, self.lo].astype(F32)
            hi = got[:, self.h:] + self.r1l[s, a, self.hi].astype(F32) + self.r2r[s, a, :].astype(F32)
            total = jnp.concatenate([lo, hi], axis=1).astype(BF16)
            self.mine[s, a, :] = self.finish(i, a, total)
            return 0

        lax.fori_loop(0, r // 16, add, 0)
        for copy in self.own(i):
            copy.start()
        self.keep(i).start()

    def s4(self, i):
        copies = self.own(i)
        for copy in copies:
            copy.wait_send()
        copies[0].wait_recv()
        copies[1].wait_recv()
        for copy in self.onward(i):
            copy.start()
        for copy in self.across(i):
            copy.start()

    def s5(self, i):
        for copy in self.onward(i):
            copy.wait()
        self.last(i).start()

    def s6(self, i):
        self.own(i)[2].wait_recv()
        for copy in self.across(i):
            copy.wait()
        self.last(i).wait()
        self.keep(i).wait()


def _layer_kernel(m, l1_ref, x_hbm, g1_ref, g2_ref, cos_hbm, sin_hbm, wq_hbm, wk_hbm, wv_hbm, wo_hbm, wg_hbm, wu_hbm, wd_hbm,
                  y_hbm, b_hbm, k_hbm, v_hbm,
                  wq_buf, wkv_buf, wo_buf, cos_buf, sin_buf, q_buf, k_buf, v_buf, vt_buf, s_buf, acc_buf, o_buf,
                  x_buf, h_buf, xb_buf, u_buf, wgu_buf, wd_buf,
                  part, p_got, p_r1l, p_r1r, p_r2l, p_r2r, p_mine,
                  r_got, r_r1l, r_r1r, r_r2l, r_r2r, r_mine,
                  p_sems, r_sems, sems, wgu_sems, wd_sems):
    n, d = x_hbm.shape
    f = wg_hbm.shape[1]
    ft, dt = wgu_buf.shape[2] // 2, wd_buf.shape[2]
    nf, nd, nc = f // ft, d // dt, n // m
    ot = 1024
    r = m // 8

    def finish_p(i, a, total):
        xf = x_buf[a, :].astype(F32) + total.astype(F32)
        h = xf.astype(BF16)
        h_buf[i, a, :] = h
        hf = h.astype(F32)
        ms = jnp.mean(hf * hf, axis=-1, keepdims=True)
        return (hf * lax.rsqrt(ms + EPS) * g2_ref[...].astype(F32)[None]).astype(BF16)

    def finish_r(i, a, total):
        return (h_buf[i, a, :].astype(F32) + total.astype(F32)).astype(BF16)

    ps = _Stream(m, part, p_got, p_r1l, p_r1r, p_r2l, p_r2r, p_mine, b_hbm, p_sems, finish_p)
    rs = _Stream(m, part, r_got, r_r1l, r_r1r, r_r2l, r_r2r, r_mine, y_hbm, r_sems, finish_r)

    barrier = pltpu.get_barrier_semaphore()
    for to in (ps.right, ps.left, ps.twin):
        pl.semaphore_signal(barrier, inc=1, device_id={"tp": to}, device_id_type=pl.DeviceIdType.MESH)
    pl.semaphore_wait(barrier, 3)

    def wgu(k, s):
        c = _cols(k, ft)
        return (pltpu.make_async_copy(wg_hbm.at[:, c], wgu_buf.at[s, :, pl.ds(0, ft)], wgu_sems.at[s, 0]),
                pltpu.make_async_copy(wu_hbm.at[:, c], wgu_buf.at[s, :, pl.ds(ft, ft)], wgu_sems.at[s, 1]))

    def wd(k, s):
        return pltpu.make_async_copy(wd_hbm.at[:, _cols(k, dt)], wd_buf.at[s], wd_sems.at[s])

    def load_chunk(i):
        r = _rows(i, m)
        t = _rows(i % (nc // 2), m)
        return (pltpu.make_async_copy(x_hbm.at[r, :], xb_buf, sems.at[0]),
                pltpu.make_async_copy(cos_hbm.at[t, :], cos_buf, sems.at[4]),
                pltpu.make_async_copy(sin_hbm.at[t, :], sin_buf, sems.at[5]))

    def store_kv(i):
        r = _rows(i, m)
        return (pltpu.make_async_copy(k_buf.at[r, :], k_hbm.at[r, :], sems.at[6]),
                pltpu.make_async_copy(v_buf, v_hbm.at[r, :], sems.at[7]))

    def load_x(i):
        return pltpu.make_async_copy(x_hbm.at[ps.place(i, ps.x), :], x_buf, sems.at[1])

    def load_b(i):
        return pltpu.make_async_copy(b_hbm.at[_rows(i, m), :], xb_buf, sems.at[2])

    heads = wq_hbm.shape[1] // HEAD
    head = _cols(lax.axis_index("tp"), HEAD)
    load_wo = pltpu.make_async_copy(wo_hbm, wo_buf, sems.at[3])
    load_qkv = (pltpu.make_async_copy(wk_hbm.at[:, head], wkv_buf.at[:, pl.ds(0, HEAD)], sems.at[8]),
                pltpu.make_async_copy(wv_hbm.at[:, head], wkv_buf.at[:, pl.ds(HEAD, HEAD)], sems.at[9]),
                pltpu.make_async_copy(wq_hbm, wq_buf, sems.at[10]))
    for copy in (*load_chunk(0), *load_qkv):
        copy.start()

    def gate_up(i, lo, hi):
        def tile(k, _):
            at = i * nf + k
            s = at % 2
            for copy in wgu(k, s):
                copy.wait()
            z = _dot(xb_buf[...], wgu_buf[s])
            gate = z[:, :ft].astype(BF16).astype(F32)
            up = z[:, ft:].astype(BF16).astype(F32)
            u_buf[:, _cols(k, ft)] = (gate * (1.0 / (1.0 + jnp.exp(-gate))) * up).astype(BF16)

            @pl.when(at + 2 < nc * nf)
            def _():
                for copy in wgu((k + 2) % nf, s):
                    copy.start()
            return 0

        lax.fori_loop(lo, hi, tile, 0)

    def down(i, lo, hi):
        def tile(k, _):
            at = i * nd + k
            s = at % 2
            wd(k, s).wait()
            part[:, _cols(k, dt)] = _dot(u_buf[...], wd_buf[s]).astype(BF16)

            @pl.when(at + 2 < nc * nd)
            def _():
                wd((k + 2) % nd, s).start()
            return 0

        lax.fori_loop(lo, hi, tile, 0)

    def project(i):
        for copy in load_chunk(i):
            copy.wait()
        _norm_chunk(m, xb_buf, g1_ref[...].astype(F32)[None], xb_buf)

        @pl.when(i == 0)
        def _():
            for copy in load_qkv:
                copy.wait()
            load_wo.start()
            for k in range(2):
                for copy in wgu(k % nf, k):
                    copy.start()
                wd(k % nd, k).start()

        _project_chunk(i, m, i // (nc // 2), xb_buf, wq_buf, wkv_buf, cos_buf, sin_buf, q_buf, k_buf, v_buf, vt_buf)
        for copy in store_kv(i):
            copy.start()

    def attend(i):
        for h in range(0, heads, 2):
            _attend_heads(i, m, l1_ref[0], h, 2, q_buf, k_buf, vt_buf, s_buf, acc_buf, o_buf)

        @pl.when(i == 0)
        def _():
            load_wo.wait()

        def tile(k, _):
            part[:, _cols(k, ot)] = _dot(o_buf[...], wo_buf[:, _cols(k, ot)]).astype(BF16)
            return 0

        lax.fori_loop(0, d // ot, tile, 0)
        for copy in store_kv(i):
            copy.wait()

    def step(j, _):
        def at(delay):
            return lambda body: pl.when((j >= delay) & (j < nc + delay))(lambda: body(j - delay))

        at(0)(project)
        at(4)(rs.s4)
        at(3)(rs.s1)
        at(0)(attend)
        at(1)(ps.s3)
        at(0)(ps.s0)

        @at(2)
        def _(i):
            ps.s6(i)
            load_b(i).start()
            load_b(i).wait()
            gate_up(i, 0, (nf + 1) // 2)

        at(4)(rs.s5)
        at(3)(rs.s2)
        at(2)(lambda i: gate_up(i, (nf + 1) // 2, nf))

        @pl.when(j + 1 < nc)
        def _():
            for copy in load_chunk(j + 1):
                copy.start()

        at(1)(ps.s4)
        at(0)(ps.s1)
        at(2)(lambda i: down(i, 0, nd // 2))
        at(4)(rs.s6)
        at(3)(rs.s3)
        at(2)(lambda i: down(i, nd // 2, nd))
        at(1)(ps.s5)

        @at(0)
        def _(i):
            load_x(i).start()
            ps.s2(i)
            load_x(i).wait()

        at(2)(rs.s0)
        return 0

    lax.fori_loop(0, nc + 5, step, 0)


def _layer(x, lens, g1, g2, cos, sin, wq, wk, wv, wo, wg, wu, wd):
    n, d = x.shape
    m = _rows_per_chunk(n)
    r, h, hq, f = m // 8, d // 2, wq.shape[1], wg.shape[1]
    ft, dt = 256, 512
    stream = [pltpu.VMEM((2, 4 * r, d), BF16),
              pltpu.VMEM((2, r, d), BF16), pltpu.VMEM((2, r, d), BF16),
              pltpu.VMEM((2, r, h), BF16), pltpu.VMEM((2, r, h), BF16), pltpu.VMEM((2, r, d), BF16)]
    whole, head = jax.ShapeDtypeStruct((n, d), BF16), jax.ShapeDtypeStruct((n, HEAD), BF16)
    vmem = pl.BlockSpec(memory_space=pltpu.VMEM)
    return pl.pallas_call(
        functools.partial(_layer_kernel, m),
        out_shape=(whole, whole, head, head),
        in_specs=[pl.BlockSpec(memory_space=pltpu.SMEM), ANY, vmem, vmem] + [ANY] * 9,
        out_specs=(ANY,) * 4,
        scratch_shapes=[
            pltpu.VMEM((d, hq), BF16), pltpu.VMEM((d, 2 * HEAD), BF16), pltpu.VMEM((hq, d), BF16),
            pltpu.VMEM((m, HEAD), F32), pltpu.VMEM((m, HEAD), F32), pltpu.VMEM((hq // HEAD * m, HEAD), BF16),
            pltpu.VMEM((n, HEAD), BF16), pltpu.VMEM((m, HEAD), BF16), pltpu.VMEM((HEAD, n), BF16),
            pltpu.VMEM((m, 2 * m), F32), pltpu.VMEM((HEAD, 2 * m), F32), pltpu.VMEM((m, hq), BF16),
            pltpu.VMEM((r, d), BF16), pltpu.VMEM((n // m, r, d), BF16), pltpu.VMEM((m, d), BF16),
            pltpu.VMEM((m, f), BF16), pltpu.VMEM((2, d, 2 * ft), BF16), pltpu.VMEM((2, f, dt), BF16),
            pltpu.VMEM((m, d), BF16), *stream, *stream,
            pltpu.SemaphoreType.DMA((2, 2, 16)), pltpu.SemaphoreType.DMA((2, 2, 16)),
            pltpu.SemaphoreType.DMA((11,)), pltpu.SemaphoreType.DMA((2, 2)), pltpu.SemaphoreType.DMA((2,)),
        ],
        compiler_params=pltpu.CompilerParams(collective_id=0, has_side_effects=True, vmem_limit_bytes=VMEM_LIMIT),
        name="layer",
    )(lens, x, g1, g2, cos, sin, wq, wk, wv, wo, wg, wu, wd)


def _finish_kernel(m, l1_ref, y_in, k_in, v_in, y_out, ck_out, cv_out, y_buf, k_buf, v_buf, kf_buf, vf_buf, ck_buf, cv_buf,
                   in_sems, out_sems, sems):
    n = y_in.shape[0]
    nc = n // m
    l1 = l1_ref[0]
    rows = [pl.ds(i * m, m) for i in range(nc)]
    loads = [pltpu.make_async_copy(y_in.at[rows[i], :], y_buf.at[i], in_sems.at[i]) for i in range(nc)]
    stores = [pltpu.make_async_copy(y_buf.at[i], y_out.at[rows[i], :], out_sems.at[i]) for i in range(nc)]
    heads = [pltpu.make_async_copy(k_in, k_buf, sems.at[0]), pltpu.make_async_copy(v_in, v_buf, sems.at[1])]
    caches = [pltpu.make_async_copy(ck_buf, ck_out, sems.at[2]), pltpu.make_async_copy(cv_buf, cv_out, sems.at[3])]
    for copy in heads + loads:
        copy.start()
    for copy in heads:
        copy.wait()
    for src, buf in ((k_buf, kf_buf), (v_buf, vf_buf)):
        buf[pl.ds(n, m), :] = jnp.zeros((m, HEAD), F32)

        def widen(i, _):
            buf[_rows(i, m), :] = src[_rows(i, m), :].astype(F32)
            return 0

        lax.fori_loop(0, nc, widen, 0)
    for i in range(nc):
        loads[i].wait()
        stores[i].start()
        at = i * m + lax.broadcasted_iota(jnp.int32, (m, 1), 0)
        start = jnp.minimum(l1 + i * m, n)
        for buf, out in ((kf_buf, ck_buf), (vf_buf, cv_buf)):
            out[0, rows[i], :] = jnp.where(at < l1, buf[rows[i], :], 0.0).astype(BF16)
            out[1, rows[i], :] = jnp.where(at < n - l1, buf[pl.ds(start, m), :], 0.0).astype(BF16)
    for copy in caches:
        copy.start()
    for copy in caches + stores:
        copy.wait()


def _finish(lens, y, k, v):
    n, d = y.shape
    m = _rows_per_chunk(n)
    cache = jax.ShapeDtypeStruct((2, n, HEAD), BF16)
    return pl.pallas_call(
        functools.partial(_finish_kernel, m),
        out_shape=(jax.ShapeDtypeStruct((n, d), BF16), cache, cache),
        in_specs=[pl.BlockSpec(memory_space=pltpu.SMEM), ANY, ANY, ANY],
        out_specs=(ANY,) * 3,
        scratch_shapes=[pltpu.VMEM((n // m, m, d), BF16), pltpu.VMEM((n, HEAD), BF16), pltpu.VMEM((n, HEAD), BF16),
                        pltpu.VMEM((n + m, HEAD), F32), pltpu.VMEM((n + m, HEAD), F32),
                        pltpu.VMEM((2, n, HEAD), BF16), pltpu.VMEM((2, n, HEAD), BF16),
                        pltpu.SemaphoreType.DMA((n // m,)), pltpu.SemaphoreType.DMA((n // m,)), pltpu.SemaphoreType.DMA((4,))],
        compiler_params=pltpu.CompilerParams(vmem_limit_bytes=VMEM_LIMIT),
        name="finish",
    )(lens, y, k, v)


def solution(mesh):
    assert mesh.shape["tp"] == 8

    def layer(x, lens, g1, g2, wq, wk, wv, wo, wg, wu, wd):
        n, d = x.shape
        l1 = lens[0]
        rows = jnp.arange(n)
        pos = jnp.where(rows >= l1, rows - l1, rows)
        inv = BASE ** (-jnp.arange(0, HEAD, 2, dtype=F32) / HEAD)
        pos = pos.astype(F32).reshape(2, n // 2, 1)
        ang = jnp.where(jnp.arange(HEAD) < HEAD // 2, pos[0], pos[1]) * jnp.concatenate([inv, inv])
        cos, sin = jnp.cos(ang), jnp.sin(ang)
        y, _, k, v = _layer(x, lens, g1, g2, cos, sin, wq, wk, wv, wo, wg, wu, wd)
        y, ck, cv = _finish(lens, y, k, v)
        return y, ck[:, :, None, :], cv[:, :, None, :]

    row = P("dp", None)
    cache = P("dp", None, "tp", None)
    return jax.shard_map(
        layer, mesh=mesh,
        in_specs=(row, P("dp"), P(), P(), P(None, "tp"), P(), P(), P("tp", None),
                  P(None, "tp"), P(None, "tp"), P("tp", None)),
        out_specs=(row, cache, cache), check_vma=False)
```
